32 devices in a mesh: pair: 2 (over y), rep: 4 (over x, core), blk: 4 (over z).
Axes of the slice: x: 2, y: 2, z: 4, core: 2. Of those that a mesh axis runs over, the one named last changes fastest.
Arguments:
- src_spectra: bfloat16 [64, 8192], P(None, ('pair', 'rep', 'blk')), parts along dimension 1, may hold values from -4 to 4
- tgt_spectra: bfloat16 [64, 8192], P(None, ('pair', 'blk')), parts along dimension 1, may hold values from -4 to 4
- log_src_weight: float32 [8192], P(('pair', 'rep', 'blk')), parts along dimension 0, may hold values from -2 to 2
- log_tgt_weight: float32 [8192], P(('pair', 'blk')), parts along dimension 0, may hold values from -2 to 2
- src_potential: float32 [8192], P(('pair', 'rep', 'blk')), parts along dimension 0, may hold values from -4 to 250
- tgt_potential: float32 [8192], P(('pair', 'blk')), parts along dimension 0, may hold values from -4 to 250
Outputs:
- src_updated: float32 [8192], P(('pair', 'rep', 'blk')), parts along dimension 0
- tgt_updated: float32 [8192], P(('pair', 'blk')), parts along dimension 0
The draws below stay inside these ranges and needn't reach their ends.
There are 2 independent parts, one for each index of `pair`. The reference program is written for one: setup_inputs(seed, part) draws one part's arguments, and reference() takes and returns one part's arrays. A program takes and returns all parts, laid end to end along the dimension named above; each array names one. Nothing has to cross between parts.
All inputs are finite; a program needn't handle non-finite values.
Results may differ from the reference program's by a relative error of at most 0.0003.
Values may be sent and summed in bfloat16 or wider, within the bound.
No kernel may reach another device: no remote copies, remote signals or barrier semaphores. Data moves between devices by JAX's collectives and lax.ppermute only.
A program may use at most 128 MiB of HBM per device.

```python
import jax
import jax.numpy as jnp
from jax import lax

C = 64
PIXELS = 4096


def spectra(key, salt):
    base = jax.random.fold_in(key, salt)
    values = jnp.clip(0.35 * jax.random.normal(base, (C, PIXELS), jnp.float32), -4.0, 4.0)
    return values


def potential(key, salt):
    base = jax.random.fold_in(key, salt)
    values = jnp.clip(jax.random.normal(base, (PIXELS,), jnp.float32), -4.0, 4.0)
    return values


def draw_src_spectra(key, part):
    return spectra(key, 11).astype(jnp.bfloat16)


def draw_tgt_spectra(key, part):
    return spectra(key, 23).astype(jnp.bfloat16)


def draw_src_potential(key, part):
    return potential(key, 37)


def draw_tgt_potential(key, part):
    return potential(key, 41)


def shard_levels(stream_key, shape, shards, smallest, largest):
    def one(axis_at, shards_of):
        draws = jax.random.uniform(jax.random.fold_in(jax.random.fold_in(stream_key, 6), axis_at), (shards_of,), jnp.float32, smallest / len(shards), largest / len(shards))
        return jnp.repeat(jnp.exp(draws), shape[axis_at] // shards_of).reshape((-1,) + (1,) * (len(shape) - axis_at - 1))

    factor_of = one(*shards[0])
    for cut in shards[1:]:
        factor_of = factor_of * one(*cut)
    return factor_of


def setup_inputs(seed: int = 0, part: int = 0) -> dict:
    streams_of = jax.random.split(jax.random.key(seed), 7)
    part_splits = jax.random.split(jax.random.fold_in(streams_of[6], part), 7)
    return {
        "src_spectra": draw_src_spectra(jax.random.fold_in(jax.random.fold_in(streams_of[6], part), 71), part),
        "tgt_spectra": draw_tgt_spectra(jax.random.fold_in(jax.random.fold_in(streams_of[6], part), 71), part),
        "log_src_weight": jnp.clip(jax.random.uniform(part_splits[2], (PIXELS,), jnp.float32, -2.0, 2.0) * shard_levels(part_splits[2], (PIXELS,), ((0, 16),), -0.4, 0.0), -2.0, 2.0),
        "log_tgt_weight": jnp.clip(jax.random.uniform(part_splits[3], (PIXELS,), jnp.float32, -2.0, 2.0) * shard_levels(part_splits[3], (PIXELS,), ((0, 4),), -0.4, 0.0), -2.0, 2.0),
        "src_potential": draw_src_potential(jax.random.fold_in(jax.random.fold_in(streams_of[6], part), 71), part),
        "tgt_potential": draw_tgt_potential(jax.random.fold_in(jax.random.fold_in(streams_of[6], part), 71), part),
    }


def reference(src_spectra, tgt_spectra, log_src_weight, log_tgt_weight, src_potential, tgt_potential):
    src_float = src_spectra.astype(jnp.float32)
    tgt_float = tgt_spectra.astype(jnp.float32)
    src_square = 0.5 * jnp.sum(src_float * src_float, axis=0)
    tgt_square = 0.5 * jnp.sum(tgt_float * tgt_float, axis=0)
    src_bias = log_src_weight + src_potential
    tgt_bias = log_tgt_weight + tgt_potential
    count = src_spectra.shape[1]
    rows_block = 512 if count % 512 == 0 else count
    blocks = count // rows_block

    def absorb(carry, block_index):
        col_peak, col_totals = carry
        offset = (block_index * rows_block).astype(jnp.int32)
        block = lax.dynamic_slice_in_dim(src_spectra, offset, rows_block, 1)
        square = lax.dynamic_slice_in_dim(src_square, offset, rows_block, 0)
        bias = lax.dynamic_slice_in_dim(src_bias, offset, rows_block, 0)
        products = lax.dot_general(block, tgt_spectra, (((0,), (0,)), ((), ())), preferred_element_type=jnp.float32)
        cost_tile = square[:, None] + tgt_square[None, :] - products
        row_scores = tgt_bias[None, :] - cost_tile
        row_peak = jnp.max(row_scores, axis=1)
        src_new = -(row_peak + jnp.log(jnp.sum(jnp.exp(row_scores - row_peak[:, None]), axis=1)))
        col_scores = bias[:, None] - cost_tile
        block_peak = jnp.max(col_scores, axis=0)
        block_totals = jnp.sum(jnp.exp(col_scores - block_peak[None, :]), axis=0)
        joined = jnp.maximum(col_peak, block_peak)
        col_totals = col_totals * jnp.exp(col_peak - joined) + block_totals * jnp.exp(block_peak - joined)
        return (joined, col_totals), src_new

    start_peak = jnp.full((count,), -jnp.inf, jnp.float32)
    start_totals = jnp.zeros((count,), jnp.float32)
    (col_peak, col_totals), src_blocks = lax.scan(absorb, (start_peak, start_totals), jnp.arange(blocks, dtype=jnp.int32))
    src_new = src_blocks.reshape(-1)
    tgt_new = -(col_peak + jnp.log(col_totals))
    return 0.5 * (src_potential + src_new), 0.5 * (tgt_potential + tgt_new)
```

```python
import functools

import jax
import jax.numpy as jnp
from jax import lax
from jax.experimental import pallas as pl
from jax.experimental.pallas import tpu as pltpu
from jax.sharding import PartitionSpec as P

EXTRA = 8


def partners(axis):
    count = lax.axis_size(axis)
    if count & (count - 1) == 0:
        return [[(i, i ^ s) for i in range(count)] for s in range(count - 1, 0, -1)]
    return [[(i, (i + s) % count) for i in range(count)] for s in range(1, count)]


def back(pattern):
    return [(target, source) for source, target in pattern]


def three_parts(value):
    high = value.astype(jnp.bfloat16).astype(jnp.float32)
    rest = value - high
    middle = rest.astype(jnp.bfloat16).astype(jnp.float32)
    low = (rest - middle).astype(jnp.bfloat16).astype(jnp.float32)
    return high, middle, low


def extra_rows(width, rows):
    index = lax.broadcasted_iota(jnp.int32, (EXTRA, width), 0)
    block = jnp.zeros((EXTRA, width), jnp.float32)
    for at, row in rows.items():
        block = jnp.where(index == at, row, block)
    return block.astype(jnp.bfloat16)


def half_square(spectra):
    wide = spectra.astype(jnp.float32)
    return 0.5 * jnp.sum(wide * wide, axis=0, keepdims=True)


def pack_kernel(spectra_ref, weight_ref, potential_ref, packed_ref):
    bands, width = spectra_ref.shape
    spectra = spectra_ref[...]
    bias = weight_ref[...] + potential_ref[...] - half_square(spectra)
    high, middle, low = three_parts(bias)
    packed_ref[:bands, :] = spectra
    packed_ref[bands:, :] = extra_rows(
        width, {0: high, 1: middle, 2: low, 3: 1.0, 4: 1.0, 5: 1.0}
    )


def log_sum(scores):
    peak = jnp.max(scores, axis=0, keepdims=True)
    return peak, jnp.sum(jnp.exp(scores - peak), axis=0, keepdims=True)


def tile_stats(packed, turned, col_operand):
    row_scores = jnp.dot(turned, packed, preferred_element_type=jnp.float32)
    row_peak, row_total = log_sum(row_scores)
    col_scores = lax.dot_general(
        packed, col_operand, (((0,), (0,)), ((), ())), preferred_element_type=jnp.float32
    )
    return row_peak + jnp.log(row_total), log_sum(col_scores)


def merge_parts(parts):
    peak = functools.reduce(jnp.maximum, [part[0] for part in parts])
    return peak, sum(part[1] * jnp.exp(part[0] - peak) for part in parts)


def home_kernel(
    packed_ref, spectra_ref, weight_ref, potential_ref, src_spectra_ref, src_potential_ref,
    turned_ref, operand_ref, rows_ref, col_peak_ref, col_total_ref, src_base_ref, tgt_base_ref,
):
    bands, width = spectra_ref.shape
    spectra = spectra_ref[...]
    square = half_square(spectra)
    high, middle, low = three_parts(weight_ref[...] + potential_ref[...] - square)
    row_operand = jnp.concatenate(
        [spectra, extra_rows(width, {3: high, 4: middle, 5: low})], axis=0
    )
    turned_ref[...] = row_operand.T
    operand_ref[:bands, :] = spectra
    operand_ref[bands:, :] = extra_rows(width, {0: 1.0, 1: 1.0, 2: 1.0})
    rows, (peak, total) = tile_stats(packed_ref[...], turned_ref[...], operand_ref[...])
    rows_ref[...] = rows
    col_peak_ref[...] = peak
    col_total_ref[...] = total
    src_base_ref[...] = src_potential_ref[...] + half_square(src_spectra_ref[...])
    tgt_base_ref[...] = potential_ref[...] + square


def away_kernel(turned_ref, operand_ref, col_peak_ref, col_total_ref, *refs):
    count = (len(refs) - 1) // 2
    parts = [(col_peak_ref[...], col_total_ref[...])]
    for packed_ref, rows_ref in zip(refs[:count], refs[count : 2 * count]):
        rows, part = tile_stats(packed_ref[...], turned_ref[...], operand_ref[...])
        rows_ref[...] = rows
        parts.append(part)
    peak, total = merge_parts(parts)
    refs[-1][...] = peak + jnp.log(total)


def joined_logs(logs):
    peak = functools.reduce(jnp.maximum, logs)
    return peak + jnp.log(sum(jnp.exp(log - peak) for log in logs))


def final_kernel(rows_count, src_base_ref, tgt_base_ref, *refs):
    logs, (src_ref, tgt_ref) = [ref[...] for ref in refs[:-2]], refs[-2:]
    src_ref[...] = 0.5 * (src_base_ref[...] - joined_logs(logs[:rows_count]))
    tgt_ref[...] = 0.5 * (tgt_base_ref[...] - joined_logs(logs[rows_count:]))


def cost(flops):
    return pl.CostEstimate(flops=flops, bytes_accessed=1 << 18, transcendentals=1 << 18)


def on_device(
    src_spectra, tgt_spectra, log_src_weight, log_tgt_weight, src_potential, tgt_potential
):
    bands, rows = src_spectra.shape
    columns = tgt_spectra.shape[1]
    depth = bands + EXTRA
    f32 = functools.partial(jax.ShapeDtypeStruct, dtype=jnp.float32)
    bf16 = functools.partial(jax.ShapeDtypeStruct, dtype=jnp.bfloat16)
    flat = lambda value: value.reshape(1, -1)
    tile_flops = 4 * rows * columns * depth

    packed = pl.pallas_call(pack_kernel, out_shape=bf16((depth, rows)))(
        src_spectra, flat(log_src_weight), flat(src_potential)
    )
    patterns = partners("blk")
    arrived = [lax.ppermute(packed, "blk", pattern) for pattern in patterns]
    turned, operand, home_rows, peak, total, src_base, tgt_base = pl.pallas_call(
        home_kernel,
        out_shape=(
            bf16((columns, depth)), bf16((depth, columns)), f32((1, rows)),
            f32((1, columns)), f32((1, columns)), f32((1, rows)), f32((1, columns)),
        ),
        cost_estimate=cost(tile_flops),
    )(packed, tgt_spectra, flat(log_tgt_weight), flat(tgt_potential), src_spectra, flat(src_potential))
    *away_rows, col_logs = pl.pallas_call(
        away_kernel,
        out_shape=tuple(f32((1, rows)) for _ in arrived) + (f32((1, columns)),),
        cost_estimate=cost(tile_flops * max(1, len(arrived))),
    )(turned, operand, peak, total, *arrived)
    row_logs = [home_rows] + [
        lax.ppermute(value, "blk", back(pattern)) for value, pattern in zip(away_rows, patterns)
    ]
    copies = lax.axis_size("rep")
    if copies & (copies - 1) == 0:
        last = [col_logs]
        step = 1
        while step < copies:
            held = last[0] if len(last) == 1 else joined_logs(last)
            last = [held, lax.ppermute(held, "rep", [(i, i ^ step) for i in range(copies)])]
            step *= 2
    else:
        last = [col_logs] + [lax.ppermute(col_logs, "rep", p) for p in partners("rep")]
    src_updated, tgt_updated = pl.pallas_call(
        functools.partial(final_kernel, len(row_logs)),
        out_shape=(f32((1, rows)), f32((1, columns))),
    )(src_base, tgt_base, *row_logs, *last)
    return src_updated.reshape(-1), tgt_updated.reshape(-1)


def solution(mesh):
    placed = (
        P(None, ("pair", "rep", "blk")),
        P(None, ("pair", "blk")),
        P(("pair", "rep", "blk")),
        P(("pair", "blk")),
        P(("pair", "rep", "blk")),
        P(("pair", "blk")),
    )
    return jax.shard_map(
        on_device,
        mesh=mesh,
        in_specs=placed,
        out_specs=(P(("pair", "rep", "blk")), P(("pair", "blk"))),
        check_vma=False,
    )
```

```python
import functools

import jax
import jax.numpy as jnp
from jax import lax
from jax.experimental import pallas as pl
from jax.experimental.pallas import tpu as pltpu
from jax.sharding import PartitionSpec as P

EXTRA = 8
PHASE1 = (3, 1, 2)
BASIS = (1, 2)
VMEM = pl.BlockSpec(memory_space=pltpu.VMEM)
HBM = pl.BlockSpec(memory_space=pltpu.HBM)


def three_parts(value):
    high = value.astype(jnp.bfloat16).astype(jnp.float32)
    rest = value - high
    middle = rest.astype(jnp.bfloat16).astype(jnp.float32)
    low = (rest - middle).astype(jnp.bfloat16).astype(jnp.float32)
    return high, middle, low


def extra_rows(width, rows):
    index = lax.broadcasted_iota(jnp.int32, (EXTRA, width), 0)
    block = jnp.zeros((EXTRA, width), jnp.float32)
    for at, row in rows.items():
        block = jnp.where(index == at, row, block)
    return block.astype(jnp.bfloat16)


def half_square(spectra):
    wide = spectra.astype(jnp.float32)
    return 0.5 * jnp.sum(wide * wide, axis=0, keepdims=True)


def pack_kernel(spectra_hbm, weight_hbm, potential_hbm, packed_ref, base_ref, spectra_ref, weight_ref, potential_ref, sems):
    copies = [
        pltpu.make_async_copy(source, target, sems.at[at])
        for at, (source, target) in enumerate(
            ((spectra_hbm, spectra_ref), (weight_hbm, weight_ref), (potential_hbm, potential_ref))
        )
    ]
    for copy in copies:
        copy.start()
    for copy in copies:
        copy.wait()
    bands, width = spectra_ref.shape
    spectra = spectra_ref[...]
    square = half_square(spectra)
    bias = weight_ref[...] + potential_ref[...] - square
    high, middle, low = three_parts(bias)
    packed_ref[:bands, :] = spectra
    packed_ref[bands:, :] = extra_rows(
        width, {0: high, 1: middle, 2: low, 3: 1.0, 4: 1.0, 5: 1.0}
    )
    base_ref[...] = potential_ref[...] + square


def log_sum(blocks):
    peaks, totals = [], []
    for scores in blocks:
        folded = scores.reshape(-1, 8, scores.shape[1])
        peak = jnp.max(folded, axis=0)
        peaks.append(peak)
        totals.append(jnp.sum(jnp.exp(folded - peak[None]), axis=0))
    top = jnp.max(functools.reduce(jnp.maximum, peaks), axis=0, keepdims=True)
    total = sum(total * jnp.exp(peak - top) for peak, total in zip(peaks, totals))
    return top, jnp.sum(total, axis=0, keepdims=True)


def pieces(length, size=256):
    return [slice(at, min(at + size, length)) for at in range(0, length, size)]


def row_logs_of(packed, turned_ref):
    blocks = [
        jnp.dot(turned_ref[piece, :], packed, preferred_element_type=jnp.float32)
        for piece in pieces(turned_ref.shape[0])
    ]
    peak, total = log_sum(blocks)
    return peak + jnp.log(total)


def col_part_of(packed, operand_ref):
    turned = packed.T
    parts = [
        log_sum([jnp.dot(turned, operand_ref[:, piece], preferred_element_type=jnp.float32)])
        for piece in pieces(operand_ref.shape[1], 256)
    ]
    return tuple(jnp.concatenate(part, axis=1) for part in zip(*parts))


def merge_parts(parts):
    peak = functools.reduce(jnp.maximum, [part[0] for part in parts])
    return peak, sum(part[1] * jnp.exp(part[0] - peak) for part in parts)


def home_kernel(
    packed_ref, spectra_ref, weight_ref, potential_ref,
    turned_ref, operand_ref, rows_ref, col_peak_ref, col_total_ref, base_ref,
):
    bands, width = spectra_ref.shape
    spectra = spectra_ref[...]
    square = half_square(spectra)
    high, middle, low = three_parts(weight_ref[...] + potential_ref[...] - square)
    row_operand = jnp.concatenate(
        [spectra, extra_rows(width, {3: high, 4: middle, 5: low})], axis=0
    )
    turned_ref[...] = row_operand.T
    operand_ref[:bands, :] = spectra
    operand_ref[bands:, :] = extra_rows(width, {0: 1.0, 1: 1.0, 2: 1.0})
    packed = packed_ref[...]
    rows_ref[...] = row_logs_of(packed, turned_ref)
    peak, total = col_part_of(packed, operand_ref)
    col_peak_ref[...] = peak
    col_total_ref[...] = total
    base_ref[...] = potential_ref[...] + square


def rows_kernel(packed_ref, turned_ref, *refs):
    fresh = row_logs_of(packed_ref[...], turned_ref)
    refs[-1][0:1, :] = fresh
    for at, ref in enumerate(refs[:-1]):
        refs[-1][at + 1 : at + 2, :] = ref[...]


def give_columns(part, out_refs):
    peak, total = part
    if len(out_refs) == 1:
        out_refs[0][...] = peak + jnp.log(total)
    else:
        out_refs[0][...] = peak
        out_refs[1][...] = total


def cols_kernel(packed_ref, operand_ref, peak_ref, total_ref, *out_refs):
    part = col_part_of(packed_ref[...], operand_ref)
    give_columns(merge_parts([(peak_ref[...], total_ref[...]), part]), out_refs)


def both_kernel(packed_ref, turned_ref, operand_ref, peak_ref, total_ref, rows_ref, *out_refs):
    packed = packed_ref[...]
    rows_ref[...] = row_logs_of(packed, turned_ref)
    part = col_part_of(packed, operand_ref)
    give_columns(merge_parts([(peak_ref[...], total_ref[...]), part]), out_refs)


def fold_kernel(*refs):
    count = len(refs) // 2
    arrived = refs[count][...]
    for at, (own_ref, out_ref) in enumerate(zip(refs[:count], refs[count + 1 :])):
        out_ref[...] = joined_logs([own_ref[...], arrived[at : at + 1, :]])


def joined_logs(logs):
    peak = functools.reduce(jnp.maximum, logs)
    return peak + jnp.log(sum(jnp.exp(log - peak) for log in logs))


def final_kernel(rows_count, src_base_ref, tgt_base_ref, *refs):
    logs, (src_ref, tgt_ref) = [ref[...] for ref in refs[:-2]], refs[-2:]
    src_ref[...] = 0.5 * (src_base_ref[...] - joined_logs(logs[:rows_count]))
    tgt_ref[...] = 0.5 * (tgt_base_ref[...] - joined_logs(logs[rows_count:]))


def kernel_call(body, out_shape, flops=1 << 16, **kw):
    return pl.pallas_call(
        body,
        out_shape=out_shape,
        compiler_params=pltpu.CompilerParams(vmem_limit_bytes=16 << 20),
        cost_estimate=pl.CostEstimate(
            flops=flops, bytes_accessed=1 << 18, transcendentals=1 << 18
        ),
        **kw,
    )


def exchange(value, axis, step):
    count = lax.axis_size(axis)
    return lax.ppermute(value, axis, [(i, i ^ step) for i in range(count)])


def on_device(
    src_spectra, tgt_spectra, log_src_weight, log_tgt_weight, src_potential, tgt_potential
):
  bands, rows = src_spectra.shape
  columns = tgt_spectra.shape[1]
  depth = bands + EXTRA
  f32 = functools.partial(jax.ShapeDtypeStruct, dtype=jnp.float32)
  bf16 = functools.partial(jax.ShapeDtypeStruct, dtype=jnp.bfloat16)
  flat = lambda value: value.reshape(1, -1)
  tile_flops = 4 * rows * columns * depth
  count = lax.axis_size("blk")
  order = PHASE1 if count == 4 else range(count - 1, 0, -1)

  packed, src_base = kernel_call(
      pack_kernel,
      (bf16((depth, rows)), f32((1, rows))),
      in_specs=[HBM] * 3,
      scratch_shapes=[
          pltpu.VMEM((bands, rows), jnp.bfloat16),
          pltpu.VMEM((1, rows), jnp.float32),
          pltpu.VMEM((1, rows), jnp.float32),
          pltpu.SemaphoreType.DMA((3,)),
      ],
  )(*(pltpu.with_memory_space_constraint(v, pltpu.HBM) for v in (src_spectra, flat(log_src_weight), flat(src_potential))))
  arrived = {step: exchange(packed, "blk", step) for step in order}
  turned, operand, home_rows, peak, total, tgt_base = kernel_call(
      home_kernel,
      (
          bf16((columns, depth)), bf16((depth, columns)), f32((1, rows)),
          f32((1, columns)), f32((1, columns)), f32((1, columns)),
      ),
      tile_flops,
  )(packed, tgt_spectra, flat(log_tgt_weight), flat(tgt_potential))
  held = [peak, total]
  logs = {0: home_rows}
  bits = list(BASIS) if count == 4 else [1 << at for at in range(count.bit_length() - 1)]
  lead = [step for step in order if step & bits[0]]
  rest_steps = [step for step in order if not step & bits[0]]
  col_shapes = lambda last: (f32((1, columns)),) * (1 if last else 2)

  def both(step, last):
      rows_out, *cols_out = kernel_call(
          both_kernel, (f32((1, rows)),) + col_shapes(last), tile_flops
      )(arrived[step], turned, operand, *held)
      return rows_out, cols_out

  def cols(step, last):
      return kernel_call(cols_kernel, col_shapes(last), tile_flops // 2)(
          arrived[step], operand, *held
      )

  def rows_of(step, *more):
      return kernel_call(rows_kernel, f32((1 + len(more), rows)), tile_flops // 2)(
          arrived[step], turned, *more
      )

  for step in lead[:-1]:
      logs[step], held = both(step, False)
  keys = [lead[-1]] + lead[:-1]
  parcel = rows_of(lead[-1], *(logs.pop(step) for step in lead[:-1]))
  landed = exchange(parcel, "blk", bits[0])
  held = cols(lead[-1], not rest_steps)
  for step in rest_steps[:-1]:
      logs[step], held = both(step, False)
  if rest_steps:
      held = cols(rest_steps[-1], True)
  here = held[0]
  there = exchange(here, "rep", 1)
  if rest_steps:
      logs[rest_steps[-1]] = rows_of(rest_steps[-1])
  here = joined_logs([here, there])
  col_logs = [here, exchange(here, "rep", 2)]
  for at, bit in enumerate(bits):
      own = [logs[key ^ bit] for key in keys]
      home_at = keys.index(bit)
      if len(bits) == at + 1:
          row_logs = [own[0], landed]
          break
      folded = kernel_call(fold_kernel, (f32((1, rows)),) * len(keys))(*own, landed)
      logs = {key ^ bit: value for key, value in zip(keys, folded)}
      keys = [key for key in logs if key & bits[at + 1]]
      parcel = [logs[key] for key in keys]
      parcel = parcel[0] if len(parcel) == 1 else jnp.concatenate(parcel, axis=0)
      landed = exchange(parcel, "blk", bits[at + 1])
  src_updated, tgt_updated = kernel_call(
      functools.partial(final_kernel, len(row_logs)), (f32((1, rows)), f32((1, columns)))
  )(src_base, tgt_base, *row_logs, *col_logs)
  return src_updated.reshape(-1), tgt_updated.reshape(-1)


def solution(mesh):
    placed = (
        P(None, ("pair", "rep", "blk")),
        P(None, ("pair", "blk")),
        P(("pair", "rep", "blk")),
        P(("pair", "blk")),
        P(("pair", "rep", "blk")),
        P(("pair", "blk")),
    )
    return jax.shard_map(
        on_device,
        mesh=mesh,
        in_specs=placed,
        out_specs=(P(("pair", "rep", "blk")), P(("pair", "blk"))),
        check_vma=False,
    )
```
